32 devices in a mesh: dp: 2 (over x), seq: 4 (over z), tensor: 4 (over y, core).
Axes of the slice: x: 2, y: 2, z: 4, core: 2. Of those that a mesh axis runs over, the one named last changes fastest.
Arguments:
- image_states: bfloat16 [2, 2048, 3072], P('dp', 'seq', 'tensor'), may hold values from -6 to 6
- text_states: bfloat16 [4, 256, 3072], P(None, 'seq', 'tensor'), may hold values from -6 to 6
- image_qkv: bfloat16 [3072, 3, 3072], P(None, None, 'tensor'), may hold values from -0.109375 to 0.109375
- text_qkv: bfloat16 [3072, 3, 3072], P(None, None, 'tensor'), may hold values from -0.109375 to 0.109375
- image_out: bfloat16 [3072, 3072], P('tensor'), may hold values from -0.109375 to 0.109375
- final_weight: bfloat16 [3072, 64], replicated, may hold values from -0.109375 to 0.109375
- query_gain: float32 [128], replicated, may hold values from 1.5 to 2.5
- key_gain: float32 [128], replicated, may hold values from 1.5 to 2.5
- modulation: float32 [10, 7, 3072], replicated, may hold values from -3 to 3
- latent: float32 [2, 2048, 64], P('dp', ('seq', 'tensor')), may hold values from -6 to 6
- old_velocity: bfloat16 [2, 2048, 64], P('dp', ('seq', 'tensor')), may hold values from -6 to 6
- rollout_noise: float32 [2, 2048, 64], P('dp', ('seq', 'tensor')), may hold values from -6 to 6
- group_ids: int32 [2], P('dp'), may hold values from 0 to 3
- text_lengths: int32 [4], replicated, may hold values from 64 to 256
- step_ids: int32 [2], P('dp'), may hold values from 0 to 9
Outputs:
- step_mean: float32 [2, 2048, 64], P('dp', ('seq', 'tensor'))
- log_ratio: float32 [2], P('dp')
The draws below stay inside these ranges and needn't reach their ends.
All inputs are finite; a program needn't handle non-finite values.
Results may differ from the reference program's by a relative error of at most 0.0023.
Values may be sent and summed in bfloat16 or wider, within the bound.
A program may use at most 192 MiB of HBM per device.

```python
import math
import jax
import jax.numpy as jnp
from jax import lax

D = 3072
HEADS = 24
HEAD_DIM = 128
CH = 64
STEPS_ALL = 10
PROMPTS = 4
IMG = 2048
TXT = 256
SAMPLES = 2


def touch_ends(array, own_key, smallest, largest):
    longest = array.shape.index(max(array.shape))
    spots = []
    for shift in (0, 1):
        where = [jax.random.randint(jax.random.fold_in(own_key, axis), (), 0, length) for axis, length in enumerate(array.shape)]
        where[longest] = (where[longest] + shift) % array.shape[longest]
        spots.append(tuple(where))
    return array.at[spots[0]].set(smallest).at[spots[1]].set(largest)


def block_levels(stream_key, extent, pieces, least, largest):
    def one(position, shards_of):
        heights = jax.random.uniform(jax.random.fold_in(jax.random.fold_in(stream_key, 6), position), (shards_of,), jnp.float32, least / len(pieces), largest / len(pieces))
        return jnp.repeat(jnp.exp(heights), extent[position] // shards_of).reshape((-1,) + (1,) * (len(extent) - position - 1))

    loudness = one(*pieces[0])
    for cut in pieces[1:]:
        loudness = loudness * one(*cut)
    return loudness


def bell_draw(key, shape, scale, bound, split=(), held_as=jnp.bfloat16):
    entries = jax.random.normal(key, shape, jnp.float32) * scale
    if len(split) > 0:
        entries = block_levels(key, shape, split, -0.22, 0.18) * entries
    return jnp.clip(entries, min=-bound, max=bound).astype(held_as)


def setup_inputs(seed: int = 0) -> dict:
    key_list = jax.random.split(jax.random.key(seed), 16)
    return {
        "image_states": bell_draw(key_list[0], (SAMPLES, IMG, D), 1.0, 6.0, ((0, 2), (1, 4), (2, 4))),
        "text_states": bell_draw(key_list[1], (PROMPTS, TXT, D), 1.0, 6.0, ((1, 4), (2, 4))),
        "image_qkv": bell_draw(key_list[2], (D, 3, D), D ** -0.5, 0.109375, ((2, 4),)),
        "text_qkv": bell_draw(key_list[3], (D, 3, D), D ** -0.5, 0.109375, ((2, 4),)),
        "image_out": bell_draw(key_list[4], (D, D), D ** -0.5, 0.109375, ((0, 4),)),
        "final_weight": bell_draw(key_list[5], (D, CH), D ** -0.5, 0.109375),
        "query_gain": jnp.clip(jax.random.uniform(key_list[6], (HEAD_DIM,), jnp.float32, 1.5, 2.5), 1.5, 2.5),
        "key_gain": jnp.clip(jax.random.uniform(key_list[7], (HEAD_DIM,), jnp.float32, 1.5, 2.5), 1.5, 2.5),
        "modulation": bell_draw(key_list[8], (STEPS_ALL, 7, D), 0.5, 3.0, (), jnp.float32),
        "latent": bell_draw(key_list[9], (SAMPLES, IMG, CH), 1.0, 6.0, ((0, 2), (1, 16)), jnp.float32),
        "old_velocity": bell_draw(key_list[10], (SAMPLES, IMG, CH), 1.0, 6.0, ((0, 2), (1, 16))),
        "rollout_noise": bell_draw(key_list[11], (SAMPLES, IMG, CH), 1.0, 6.0, ((0, 2), (1, 16)), jnp.float32),
        "group_ids": jax.random.randint(key_list[12], (SAMPLES,), 0, PROMPTS).astype(jnp.int32),
        "text_lengths": touch_ends(jax.random.randint(key_list[13], (PROMPTS,), TXT // 4, TXT + 1), jax.random.fold_in(key_list[13], 1), TXT // 4, TXT).astype(jnp.int32),
        "step_ids": jax.random.randint(key_list[14], (SAMPLES,), 0, STEPS_ALL).astype(jnp.int32),
    }


NORM_EPSILON = 1e-06
NOISE_LEVEL = 0.7

def layer_norm(values):
    row_mean = lax.optimization_barrier(jnp.mean(values, axis=-1, keepdims=True))
    centred = values - row_mean
    row_var = lax.optimization_barrier(jnp.mean(centred * centred, axis=-1, keepdims=True))
    return centred * lax.rsqrt(row_var + NORM_EPSILON)

def head_norm(values, gain_vector):
    mean_square = lax.optimization_barrier(jnp.mean(values * values, axis=-1, keepdims=True))
    return (values * lax.rsqrt(mean_square + NORM_EPSILON) * gain_vector).astype(jnp.bfloat16)

def plan(step_values, total_steps):
    step_count = total_steps + 1.0
    flow_time = (total_steps - step_values.astype(jnp.float32)) / step_count
    step_delta = -1.0 / step_count
    noise_sigma = NOISE_LEVEL * jnp.sqrt(flow_time / (1.0 - flow_time))
    spread = noise_sigma * jnp.sqrt(1.0 / step_count)
    return (flow_time, step_delta, noise_sigma, spread)

def drift_mean(latent_state, velocity, flow_time, step_delta, noise_sigma):
    drift = velocity + noise_sigma * noise_sigma / (2.0 * flow_time) * (latent_state + (1.0 - flow_time) * velocity)
    return latent_state + drift * step_delta

def reference(image_states, text_states, image_qkv, text_qkv, image_out, final_weight, query_gain, key_gain, modulation, latent, old_velocity, rollout_noise, group_ids, text_lengths, step_ids):
    score_scale = 1.0 / math.sqrt(HEAD_DIM)

    def one_sample(index):
        modrows = modulation[step_ids[index]]
        image_f = image_states[index].astype(jnp.float32)
        text_rows = text_states[group_ids[index]].astype(jnp.float32)
        normed_img = (layer_norm(image_f) * (1.0 + modrows[1]) + modrows[0]).astype(jnp.bfloat16)
        normed_txt = (layer_norm(text_rows) * (1.0 + modrows[4]) + modrows[3]).astype(jnp.bfloat16)
        qkv_img = jnp.dot(normed_img, image_qkv.reshape(D, 3 * D), preferred_element_type=jnp.float32).reshape(IMG, 3, HEADS, HEAD_DIM)
        qkv_txt = jnp.dot(normed_txt, text_qkv.reshape(D, 3 * D), preferred_element_type=jnp.float32).reshape(TXT, 3, HEADS, HEAD_DIM)
        queries = head_norm(qkv_img[:, 0], query_gain)
        key_rows = head_norm(jnp.concatenate([qkv_txt[:, 1], qkv_img[:, 1]], axis=0), key_gain)
        value_rows = jnp.concatenate([qkv_txt[:, 2], qkv_img[:, 2]], axis=0).astype(jnp.bfloat16)
        text_valid = jnp.arange(TXT, dtype=jnp.int32) < text_lengths[group_ids[index]]
        key_valid = jnp.concatenate([text_valid.astype(jnp.float32), jnp.ones((IMG,), jnp.float32)])

        def one_head(head):
            query_head = queries[:, head]
            key_head = key_rows[:, head]
            value_head = value_rows[:, head]
            scores = jnp.dot(query_head, key_head.T, preferred_element_type=jnp.float32) * score_scale
            weights = jnp.exp(scores) * key_valid[None, :]
            denominator = lax.optimization_barrier(jnp.sum(weights, axis=-1))
            numerator = jnp.dot(weights.astype(jnp.bfloat16), value_head, preferred_element_type=jnp.float32)
            return (numerator / denominator[:, None]).astype(jnp.bfloat16)
        attended = lax.map(one_head, jnp.arange(HEADS, dtype=jnp.int32))
        attended = jnp.transpose(attended, (1, 0, 2)).reshape(IMG, D)
        projected = jnp.dot(attended, image_out, preferred_element_type=jnp.float32)
        resid = image_f + modrows[2] * projected
        final_normed = (layer_norm(resid) * (1.0 + modrows[6]) + modrows[5]).astype(jnp.bfloat16)
        return jnp.dot(final_normed, final_weight, preferred_element_type=jnp.float32)
    velocity = lax.map(one_sample, jnp.arange(SAMPLES, dtype=jnp.int32))
    flow_time, step_delta, noise_sigma, spread = plan(step_ids, STEPS_ALL)
    flow_e = flow_time[:, None, None]
    sigma_e = noise_sigma[:, None, None]
    step_mean = drift_mean(latent, velocity, flow_e, step_delta, sigma_e)
    mean_old = drift_mean(latent, old_velocity.astype(jnp.float32), flow_e, step_delta, sigma_e)
    shifted = rollout_noise + (mean_old - step_mean) / spread[:, None, None]
    log_ratio = lax.optimization_barrier(jnp.sum(rollout_noise * rollout_noise - shifted * shifted, axis=(1, 2))) * 0.5 / (IMG * CH)
    return (step_mean, log_ratio)
```

```python
import functools
import math

import jax
import jax.numpy as jnp
from jax import lax
from jax.experimental import pallas as pl
from jax.experimental.pallas import tpu as pltpu
from jax.sharding import PartitionSpec as P

NORM_EPSILON = 1e-06
NOISE_LEVEL = 0.7


def layer_norm(values):
    row_mean = jnp.mean(values, axis=-1, keepdims=True)
    centred = values - row_mean
    row_var = jnp.mean(centred * centred, axis=-1, keepdims=True)
    return centred * lax.rsqrt(row_var + NORM_EPSILON)


def head_norm(values, gain_vector):
    mean_square = jnp.mean(values * values, axis=-1, keepdims=True)
    return (values * lax.rsqrt(mean_square + NORM_EPSILON) * gain_vector).astype(jnp.bfloat16)


def plan(step_values, total_steps):
    step_count = total_steps + 1.0
    flow_time = (total_steps - step_values.astype(jnp.float32)) / step_count
    step_delta = -1.0 / step_count
    noise_sigma = NOISE_LEVEL * jnp.sqrt(flow_time / (1.0 - flow_time))
    spread = noise_sigma * jnp.sqrt(1.0 / step_count)
    return (flow_time, step_delta, noise_sigma, spread)


def drift_mean(latent_state, velocity, flow_time, step_delta, noise_sigma):
    drift = velocity + noise_sigma * noise_sigma / (2.0 * flow_time) * (
        latent_state + (1.0 - flow_time) * velocity
    )
    return latent_state + drift * step_delta


MESH = pl.DeviceIdType.MESH
VMEM_LIMIT = 60 * 1024 * 1024


def first_head(rank, ranks, heads, odd):
    extra = heads % ranks
    base = heads // ranks
    even_start = base * rank + jnp.minimum(rank, extra)
    odd_start = base * rank + jnp.maximum(rank - (ranks - extra), 0)
    return jnp.where(odd == 1, odd_start, even_start)


def head_owner(head, ranks, heads, odd):
    owner = jnp.int32(0)
    for rank in range(1, ranks):
        owner = owner + (head >= first_head(jnp.int32(rank), ranks, heads, odd)).astype(jnp.int32)
    return owner, head - first_head(owner, ranks, heads, odd)


def meet(axis, size, me):
    barrier = pltpu.get_barrier_semaphore()
    for step in range(1, size):
        pl.semaphore_signal(
            barrier, inc=1, device_id={axis: lax.rem(me + step, size)}, device_id_type=MESH
        )
    pl.semaphore_wait(barrier, size - 1)


def project_kernel(
    ranks, heads, group, img_ref, txt_ref, wimg_ref, wtxt_ref, qgain_ref, kgain_ref,
    q_out, k_out, v_out, qbuf, kvbuf, send_sem, recv_sem, local_sem,
):
    me = lax.axis_index("seq")
    odd = lax.rem(lax.axis_index("tensor"), 2)
    step = pl.program_id(0)
    pieces = heads // group
    steps = 3 * pieces
    local_txt = txt_ref.shape[0]
    slots = q_out.shape[0]
    hd = qgain_ref.shape[1]
    dot = functools.partial(jnp.dot, preferred_element_type=jnp.float32)

    @pl.when(step == 0)
    def _():
        meet("seq", ranks, me)

    def normed(values, gain_ref):
        mean_square = jnp.mean(values * values, axis=-1, keepdims=True)
        return (values * lax.rsqrt(mean_square + NORM_EPSILON) * gain_ref[...]).astype(jnp.bfloat16)

    piece = lax.rem(step, pieces)
    kind = step // pieces
    img = dot(img_ref[...], wimg_ref[0])

    @pl.when(kind < 2)
    def _():
        txt = dot(txt_ref[...], wtxt_ref[0])
        for g in range(group):
            cols = slice(g * hd, (g + 1) * hd)
            head = kind * heads + piece * group + g

            @pl.when(kind == 0)
            def _():
                kvbuf[head, :local_txt, :] = normed(txt[:, cols], kgain_ref)
                kvbuf[head, local_txt:, :] = normed(img[:, cols], kgain_ref)

            @pl.when(kind == 1)
            def _():
                kvbuf[head, :local_txt, :] = txt[:, cols].astype(jnp.bfloat16)
                kvbuf[head, local_txt:, :] = img[:, cols].astype(jnp.bfloat16)

    @pl.when(kind == 2)
    def _():
        for g in range(group):
            qbuf[piece * group + g] = normed(img[:, g * hd : (g + 1) * hd], qgain_ref)

    def ship(which):
        kind_of = which // pieces
        for g in range(group):
            head = lax.rem(which, pieces) * group + g
            owner, slot = head_owner(head, ranks, heads, odd)
            for number, out in ((0, k_out), (1, v_out), (2, q_out)):
                source = qbuf.at[head] if number == 2 else kvbuf.at[number * heads + head]

                @pl.when((kind_of == number) & (owner == me))
                def _():
                    pltpu.make_async_copy(
                        source, out.at[slot, me], local_sem.at[number, slot]
                    ).start()

                @pl.when((kind_of == number) & (owner != me))
                def _():
                    pltpu.make_async_remote_copy(
                        src_ref=source,
                        dst_ref=out.at[slot, me],
                        send_sem=send_sem.at[number, head],
                        recv_sem=recv_sem.at[number, slot, me],
                        device_id={"seq": owner},
                        device_id_type=MESH,
                    ).start()

    @pl.when(step > 0)
    def _():
        ship(step - 1)

    @pl.when(step == steps - 1)
    def _():
        ship(step)
        mine = first_head(me + 1, ranks, heads, odd) - first_head(me, ranks, heads, odd)
        for number, out in ((0, k_out), (1, v_out), (2, q_out)):
            buf = qbuf if number == 2 else kvbuf

            for head in range(heads):
                owner, _ = head_owner(jnp.int32(head), ranks, heads, odd)

                @pl.when(owner != me)
                def _():
                    src = buf.at[head]
                    pltpu.make_async_remote_copy(
                        src_ref=src, dst_ref=out.at[0, me],
                        send_sem=send_sem.at[number, head], recv_sem=recv_sem.at[number, 0, me],
                        device_id={"seq": owner}, device_id_type=MESH,
                    ).wait_send()

            for slot in range(slots):
                @pl.when(slot < mine)
                def _():
                    pltpu.make_async_copy(
                        buf.at[0], out.at[slot, me], local_sem.at[number, slot]
                    ).wait()
                    for hop in range(1, ranks):
                        peer = lax.rem(me + hop, ranks)
                        pltpu.make_async_remote_copy(
                            src_ref=buf.at[0], dst_ref=out.at[slot, peer],
                            send_sem=send_sem.at[number, 0], recv_sem=recv_sem.at[number, slot, peer],
                            device_id={"seq": peer}, device_id_type=MESH,
                        ).wait_recv()


def project(ranks, heads, normed_img, normed_txt, wimg, wtxt, query_gain, key_gain):
    width = normed_img.shape[1]
    hd = query_gain.shape[0]
    group = 2 if heads % 2 == 0 else 1
    pieces = heads // group
    slots = -(-heads // ranks)
    local_img, local_txt = normed_img.shape[0], normed_txt.shape[0]
    rows = local_img + local_txt
    kv = jax.ShapeDtypeStruct((slots, ranks, rows, hd), jnp.bfloat16)
    whole = pl.BlockSpec(memory_space=pltpu.VMEM)
    return pl.pallas_call(
        functools.partial(project_kernel, ranks, heads, group),
        grid=(3 * pieces,),
        out_shape=(jax.ShapeDtypeStruct((slots, ranks, local_img, hd), jnp.bfloat16), kv, kv),
        in_specs=[
            whole,
            whole,
            pl.BlockSpec((1, width, group * hd), lambda i: ((i // pieces + 1) % 3, 0, i % pieces)),
            pl.BlockSpec(
                (1, width, group * hd),
                lambda i: (
                    jnp.minimum(i // pieces, 1), 0,
                    jnp.where(i < 2 * pieces, i % pieces, pieces - 1),
                ),
            ),
            whole,
            whole,
        ],
        out_specs=[pl.BlockSpec(memory_space=pl.ANY)] * 3,
        scratch_shapes=[
            pltpu.VMEM((heads, local_img, hd), jnp.bfloat16),
            pltpu.VMEM((2 * heads, rows, hd), jnp.bfloat16),
            pltpu.SemaphoreType.DMA((3, heads)),
            pltpu.SemaphoreType.DMA((3, slots, ranks)),
            pltpu.SemaphoreType.DMA((3, slots)),
        ],
        compiler_params=pltpu.CompilerParams(
            collective_id=0, has_side_effects=True, vmem_limit_bytes=VMEM_LIMIT,
            dimension_semantics=("arbitrary",),
        ),
    )(normed_img, normed_txt, wimg, wtxt, query_gain[None, :], key_gain[None, :])


def attend_kernel(
    ranks, heads, q_ref, k_ref, v_ref, valid_ref, out_ref, buf, send_sem, recv_sem, local_sem
):
    me = lax.axis_index("seq")
    odd = lax.rem(lax.axis_index("tensor"), 2)
    meet("seq", ranks, me)
    slots, _, local_img, hd = q_ref.shape
    start = first_head(me, ranks, heads, odd)
    mine = first_head(me + 1, ranks, heads, odd) - start
    scale = math.log2(math.e) / math.sqrt(hd)
    tile = min(256, local_img)

    def columns(head):
        return out_ref.at[:, pl.ds(pl.multiple_of(head * hd, hd), hd)]

    def back(peer, slot):
        return pltpu.make_async_remote_copy(
            src_ref=buf.at[slot, peer],
            dst_ref=columns(start + slot),
            send_sem=send_sem.at[slot, peer],
            recv_sem=recv_sem.at[start + slot],
            device_id={"seq": peer},
            device_id_type=MESH,
        )

    def place(number):
        return number // ranks, lax.rem(me + 1 + lax.rem(number, ranks), ranks)

    def ship(number):
        slot, peer = place(number)

        @pl.when((slot < mine) & (peer != me))
        def _():
            back(peer, slot).start()

        @pl.when((slot < mine) & (peer == me))
        def _():
            pltpu.make_async_copy(
                buf.at[slot, me], columns(start + slot), local_sem.at[slot]
            ).start()

    def one(number, carry):
        slot, peer = place(number)

        @pl.when(slot < mine)
        def _():
            for low in range(0, local_img, tile):
                queries = q_ref[slot, peer, low : low + tile, :]
                total = jnp.zeros((tile, hd), jnp.float32)
                denominator = jnp.zeros((tile, 1), jnp.float32)
                for block in range(ranks):
                    scores = lax.dot_general(
                        queries, k_ref[slot, block], (((1,), (1,)), ((), ())),
                        preferred_element_type=jnp.float32,
                    )
                    weights = jnp.exp2(scores * scale) * valid_ref[block]
                    denominator = denominator + jnp.sum(weights, axis=-1, keepdims=True)
                    total = total + jnp.dot(
                        weights.astype(jnp.bfloat16), v_ref[slot, block],
                        preferred_element_type=jnp.float32,
                    )
                buf[slot, peer, low : low + tile, :] = (total / denominator).astype(jnp.bfloat16)

        @pl.when(number > 0)
        def _():
            ship(number - 1)

        return carry

    lax.fori_loop(0, slots * ranks, one, 0)
    ship(slots * ranks - 1)
    for slot in range(slots):
        @pl.when(slot < mine)
        def _():
            pltpu.make_async_copy(
                buf.at[slot, me], columns(start + slot), local_sem.at[slot]
            ).wait()
            for hop in range(1, ranks):
                back(lax.rem(me + hop, ranks), slot).wait_send()

    for head in range(heads):
        owner, slot = head_owner(jnp.int32(head), ranks, heads, odd)

        @pl.when(owner != me)
        def _():
            pltpu.make_async_remote_copy(
                src_ref=buf.at[0, 0], dst_ref=columns(head), send_sem=send_sem.at[0, 0],
                recv_sem=recv_sem.at[head], device_id={"seq": owner}, device_id_type=MESH,
            ).wait_recv()


def attend(ranks, heads, queries, keys, values, valid):
    slots, _, local_img, hd = queries.shape
    vmem = pl.BlockSpec(memory_space=pltpu.VMEM)
    return pl.pallas_call(
        functools.partial(attend_kernel, ranks, heads),
        out_shape=jax.ShapeDtypeStruct((local_img, heads * hd), jnp.bfloat16),
        in_specs=[vmem] * 4,
        out_specs=pl.BlockSpec(memory_space=pl.ANY),
        scratch_shapes=[
            pltpu.VMEM((slots, ranks, local_img, hd), jnp.bfloat16),
            pltpu.SemaphoreType.DMA((slots, ranks)),
            pltpu.SemaphoreType.DMA((heads,)),
            pltpu.SemaphoreType.DMA((slots,)),
        ],
        compiler_params=pltpu.CompilerParams(
            collective_id=1, has_side_effects=True, vmem_limit_bytes=VMEM_LIMIT
        ),
    )(queries, keys, values, valid)


def reduce_kernel(
    size, att_ref, w_ref, out_ref, first, first_in, second, second_in, sems1, sems2
):
    me = lax.axis_index("tensor")
    core = lax.rem(me, 2)
    chip = me // 2
    chips = size // 2
    partner = 2 * chip + 1 - core
    rows = att_ref.shape[0] // size

    barrier = pltpu.get_barrier_semaphore()
    pl.semaphore_signal(barrier, inc=1, device_id={"tensor": partner}, device_id_type=MESH)
    for hop in range(1, chips):
        pl.semaphore_signal(
            barrier, inc=1, device_id={"tensor": 2 * lax.rem(chip + hop, chips) + core},
            device_id_type=MESH,
        )
    pl.semaphore_wait(barrier, chips)

    def partial(owner):
        block = att_ref[pl.ds(pl.multiple_of(owner * rows, rows), rows), :]
        return jnp.dot(block, w_ref[...], preferred_element_type=jnp.float32)

    def to_partner(hop):
        return pltpu.make_async_remote_copy(
            src_ref=first.at[hop], dst_ref=first_in.at[hop],
            send_sem=sems1.at[0, hop], recv_sem=sems1.at[1, hop],
            device_id={"tensor": partner}, device_id_type=MESH,
        )

    def to_chip(hop):
        return pltpu.make_async_remote_copy(
            src_ref=second.at[hop], dst_ref=second_in.at[hop],
            send_sem=sems2.at[0, hop], recv_sem=sems2.at[1, hop],
            device_id={"tensor": 2 * lax.rem(chip + hop, chips) + core}, device_id_type=MESH,
        )

    order = list(range(1, chips)) + [0]
    for hop in order:
        target = lax.rem(chip + hop, chips)
        first[hop] = partial(2 * target + 1 - core).astype(jnp.bfloat16)
        own = partial(2 * target + core)
        to_partner(hop).start()
        to_partner(hop).wait_recv()
        total = own + first_in[hop].astype(jnp.float32)
        if hop:
            second[hop] = total.astype(jnp.bfloat16)
            to_chip(hop).start()
        else:
            out_ref[...] = total
    for hop in range(1, chips):
        to_chip(hop).wait_recv()
        out_ref[...] += second_in[hop].astype(jnp.float32)
    for hop in range(chips):
        to_partner(hop).wait_send()
        if hop:
            to_chip(hop).wait_send()


def project_reduce(size, attended, image_out):
    tokens, width = attended.shape[0], image_out.shape[1]
    rows, chips = tokens // size, size // 2
    vmem = pl.BlockSpec(memory_space=pltpu.VMEM)
    stack = pltpu.VMEM((chips, rows, width), jnp.bfloat16)
    return pl.pallas_call(
        functools.partial(reduce_kernel, size),
        out_shape=jax.ShapeDtypeStruct((rows, width), jnp.float32),
        in_specs=[vmem] * 2,
        out_specs=vmem,
        scratch_shapes=[
            stack, stack, stack, stack,
            pltpu.SemaphoreType.DMA((2, chips)),
            pltpu.SemaphoreType.DMA((2, chips)),
        ],
        compiler_params=pltpu.CompilerParams(
            collective_id=2, has_side_effects=True, vmem_limit_bytes=VMEM_LIMIT
        ),
    )(attended, image_out)


def total_kernel(sizes, x_ref, out_ref, *scratch):
    me = {axis: lax.axis_index(axis) for axis, _ in sizes}
    barrier = pltpu.get_barrier_semaphore()
    count = 0
    for axis, size in sizes:
        for hop in range(1, size):
            pl.semaphore_signal(
                barrier, inc=1, device_id={axis: lax.rem(me[axis] + hop, size)},
                device_id_type=MESH,
            )
            count += 1
    pl.semaphore_wait(barrier, count)
    held = x_ref
    for number, (axis, size) in enumerate(sizes):
        slots, total, sems = scratch[3 * number : 3 * number + 3]
        copies = []
        for hop in range(1, size):
            copy = pltpu.make_async_remote_copy(
                src_ref=held, dst_ref=slots.at[hop], send_sem=sems.at[0, hop],
                recv_sem=sems.at[1, hop],
                device_id={axis: lax.rem(me[axis] + hop, size)}, device_id_type=MESH,
            )
            copy.start()
            copies.append(copy)
        sum_now = held[...]
        for hop, copy in enumerate(copies, 1):
            copy.wait()
            sum_now = sum_now + slots[hop]
        total[...] = sum_now
        held = total
    out_ref[...] = held[...]


def total_sum(sizes, tile):
    vmem = pl.BlockSpec(memory_space=pltpu.VMEM)
    scratch = []
    for _, size in sizes:
        scratch += [
            pltpu.VMEM((size,) + tile.shape, jnp.float32),
            pltpu.VMEM(tile.shape, jnp.float32),
            pltpu.SemaphoreType.DMA((2, size)),
        ]
    return pl.pallas_call(
        functools.partial(total_kernel, sizes),
        out_shape=jax.ShapeDtypeStruct(tile.shape, jnp.float32),
        in_specs=[vmem],
        out_specs=vmem,
        scratch_shapes=scratch,
        compiler_params=pltpu.CompilerParams(collective_id=3, has_side_effects=True),
    )(tile)


def gather_features(block, size):
    slot = lax.axis_index("tensor")
    chips = size // 2
    chip, core = slot // 2, lax.rem(slot, 2)
    held = [block]
    for hop in range(1, chips):
        held.append(
            lax.ppermute(
                block, "tensor",
                [(t, 2 * ((t // 2 + hop) % chips) + t % 2) for t in range(size)],
            )
        )
    other = [lax.ppermute(b, "tensor", [(t, t ^ 1) for t in range(size)]) for b in held]
    pairs = [
        jnp.where(core == 0, jnp.concatenate([a, b], axis=1), jnp.concatenate([b, a], axis=1))
        for a, b in zip(held, other)
    ]
    if chips == 2:
        return jnp.where(
            chip == 0,
            jnp.concatenate([pairs[0], pairs[1]], axis=1),
            jnp.concatenate([pairs[1], pairs[0]], axis=1),
        )
    stacked = jnp.stack(pairs)
    return jnp.concatenate([stacked[lax.rem(chip - c + chips, chips)] for c in range(chips)], axis=1)


def shards(
    image_states, text_states, image_qkv, text_qkv, image_out, final_weight, query_gain, key_gain,
    modulation, latent, old_velocity, rollout_noise, group_ids, text_lengths, step_ids,
):
    local_img = image_states.shape[1]
    local_txt = text_states.shape[1]
    hd = query_gain.shape[0]
    heads = image_qkv.shape[2] // hd
    total_steps = modulation.shape[0]
    ranks = lax.axis_size("seq")
    size = lax.axis_size("tensor")
    row_count = local_img // size
    slot = lax.axis_index("tensor")
    group = group_ids[0]
    modrows = modulation[step_ids[0]]
    length = text_lengths[group]
    joined = jnp.concatenate([text_states[group], image_states[0]], axis=0)
    full = gather_features(joined, size)
    wimg = jnp.transpose(image_qkv, (1, 0, 2))
    wtxt = jnp.transpose(text_qkv[:, 1:, :], (1, 0, 2))
    text_f = full[:local_txt].astype(jnp.float32)
    image_f = full[local_txt:].astype(jnp.float32)
    normed_img = (layer_norm(image_f) * (1.0 + modrows[1]) + modrows[0]).astype(jnp.bfloat16)
    normed_txt = (layer_norm(text_f) * (1.0 + modrows[4]) + modrows[3]).astype(jnp.bfloat16)
    queries, keys, values = project(
        ranks, heads, normed_img, normed_txt, wimg, wtxt, query_gain, key_gain
    )
    place = jnp.arange(local_txt + local_img, dtype=jnp.int32)[None, :]
    text_pos = jnp.arange(ranks, dtype=jnp.int32)[:, None] * local_txt + place
    valid = ((place >= local_txt) | (text_pos < length)).astype(jnp.float32)[:, None, :]
    attended = attend(ranks, heads, queries, keys, values, valid)
    summed = project_reduce(size, attended, image_out)
    own_rows = lax.dynamic_slice_in_dim(
        full, local_txt + slot * row_count, row_count, 0
    ).astype(jnp.float32)
    resid = own_rows + modrows[2] * summed
    final_normed = (layer_norm(resid) * (1.0 + modrows[6]) + modrows[5]).astype(jnp.bfloat16)
    velocity = jnp.dot(final_normed, final_weight, preferred_element_type=jnp.float32)[None]
    flow_time, step_delta, noise_sigma, spread = plan(step_ids, total_steps)
    flow_e = flow_time[:, None, None]
    sigma_e = noise_sigma[:, None, None]
    step_mean = drift_mean(latent, velocity, flow_e, step_delta, sigma_e)
    mean_old = drift_mean(latent, old_velocity.astype(jnp.float32), flow_e, step_delta, sigma_e)
    shifted = rollout_noise + (mean_old - step_mean) / spread[:, None, None]
    partial_ratio = jnp.sum(rollout_noise * rollout_noise - shifted * shifted) * 0.5
    tile = jnp.broadcast_to(partial_ratio, (8, 128))
    ratio_total = total_sum((("tensor", size), ("seq", ranks)), tile)[0, :1]
    elements = latent.shape[1] * ranks * size * latent.shape[2]
    return (step_mean, ratio_total / elements)


def solution(mesh):
    placed = (
        P("dp", "seq", "tensor"),
        P(None, "seq", "tensor"),
        P(None, None, "tensor"),
        P(None, None, "tensor"),
        P("tensor", None),
        P(),
        P(),
        P(),
        P(),
        P("dp", ("seq", "tensor"), None),
        P("dp", ("seq", "tensor"), None),
        P("dp", ("seq", "tensor"), None),
        P("dp"),
        P(),
        P("dp"),
    )
    return jax.shard_map(
        shards,
        mesh=mesh,
        in_specs=placed,
        out_specs=(P("dp", ("seq", "tensor"), None), P("dp")),
        check_vma=False,
    )
```

```python
import functools
import math

import jax
import jax.numpy as jnp
from jax import lax
from jax.experimental import pallas as pl
from jax.experimental.pallas import tpu as pltpu
from jax.sharding import PartitionSpec as P

NORM_EPSILON = 1e-06
NOISE_LEVEL = 0.7


def layer_norm(values):
    row_mean = jnp.mean(values, axis=-1, keepdims=True)
    centred = values - row_mean
    row_var = jnp.mean(centred * centred, axis=-1, keepdims=True)
    return centred * lax.rsqrt(row_var + NORM_EPSILON)


def head_norm(values, gain_vector):
    mean_square = jnp.mean(values * values, axis=-1, keepdims=True)
    return (values * lax.rsqrt(mean_square + NORM_EPSILON) * gain_vector).astype(jnp.bfloat16)


def plan(step_values, total_steps):
    step_count = total_steps + 1.0
    flow_time = (total_steps - step_values.astype(jnp.float32)) / step_count
    step_delta = -1.0 / step_count
    noise_sigma = NOISE_LEVEL * jnp.sqrt(flow_time / (1.0 - flow_time))
    spread = noise_sigma * jnp.sqrt(1.0 / step_count)
    return (flow_time, step_delta, noise_sigma, spread)


def drift_mean(latent_state, velocity, flow_time, step_delta, noise_sigma):
    drift = velocity + noise_sigma * noise_sigma / (2.0 * flow_time) * (
        latent_state + (1.0 - flow_time) * velocity
    )
    return latent_state + drift * step_delta


MESH = pl.DeviceIdType.MESH
VMEM_LIMIT = 60 * 1024 * 1024


def first_head(rank, ranks, heads, odd):
    extra = heads % ranks
    base = heads // ranks
    even_start = base * rank + jnp.minimum(rank, extra)
    odd_start = base * rank + jnp.maximum(rank - (ranks - extra), 0)
    return jnp.where(odd == 1, odd_start, even_start)


def head_owner(head, ranks, heads, odd):
    owner = jnp.int32(0)
    for rank in range(1, ranks):
        owner = owner + (head >= first_head(jnp.int32(rank), ranks, heads, odd)).astype(jnp.int32)
    return owner, head - first_head(owner, ranks, heads, odd)


def meet(axis, size, me):
    barrier = pltpu.get_barrier_semaphore()
    for step in range(1, size):
        pl.semaphore_signal(
            barrier, inc=1, device_id={axis: lax.rem(me + step, size)}, device_id_type=MESH
        )
    pl.semaphore_wait(barrier, size - 1)


def project_kernel(
    ranks, size, heads, local_txt, chunk, x_ref, mod_ref, wimg_hbm, wtxt_hbm, qgain_ref, kgain_ref,
    out, own_ref, gathered, normed, staged, wimg, wtxt,
    wsem, chip_send, chip_recv, core_send, core_recv, pass_send, pass_recv, own_sem,
    send_sem, recv_sem, local_sem,
):
    me = lax.axis_index("seq")
    slot_t = lax.axis_index("tensor")
    core, chip = lax.rem(slot_t, 2), slot_t // 2
    chips = size // 2
    partner = 2 * chip + 1 - core
    rows, part = x_ref.shape
    width = size * part
    hd = qgain_ref.shape[1]
    slots = out.shape[0]
    chunks = 1 + (rows - local_txt) // chunk

    def span(number):
        if number == 0:
            return pl.ds(0, local_txt)
        return pl.ds(local_txt + (number - 1) * chunk, chunk)

    def at_chip(hop):
        return 2 * lax.rem(chip + hop + chips, chips) + core

    weight_copies = (
        pltpu.make_async_copy(wtxt_hbm.at[pl.ds(1, 2)], wtxt, wsem.at[0]),
        pltpu.make_async_copy(wimg_hbm, wimg, wsem.at[1]),
    )
    for copy in weight_copies:
        copy.start()
    own_copy = pltpu.make_async_copy(x_ref, gathered.at[slot_t], own_sem)
    own_copy.start()

    barrier = pltpu.get_barrier_semaphore()
    for hop in range(1, ranks):
        pl.semaphore_signal(
            barrier, inc=1, device_id={"seq": lax.rem(me + hop, ranks)}, device_id_type=MESH
        )
    pl.semaphore_signal(barrier, inc=1, device_id={"tensor": partner}, device_id_type=MESH)
    for hop in range(1, chips):
        pl.semaphore_signal(barrier, inc=1, device_id={"tensor": at_chip(hop)}, device_id_type=MESH)
    pl.semaphore_wait(barrier, ranks - 1 + chips)

    def chip_copy(number, hop):
        return pltpu.make_async_remote_copy(
            src_ref=x_ref.at[span(number)], dst_ref=gathered.at[slot_t, span(number)],
            send_sem=chip_send.at[number, hop], recv_sem=chip_recv.at[number, hop],
            device_id={"tensor": at_chip(hop)}, device_id_type=MESH,
        )

    def core_copy(number):
        return pltpu.make_async_remote_copy(
            src_ref=x_ref.at[span(number)], dst_ref=gathered.at[slot_t, span(number)],
            send_sem=core_send.at[number], recv_sem=core_recv.at[number],
            device_id={"tensor": partner}, device_id_type=MESH,
        )

    def pass_copy(number, hop):
        block = gathered.at[at_chip(-hop), span(number)]
        return pltpu.make_async_remote_copy(
            src_ref=block, dst_ref=block,
            send_sem=pass_send.at[number, hop], recv_sem=pass_recv.at[number, hop],
            device_id={"tensor": partner}, device_id_type=MESH,
        )

    for number in range(chunks):
        for hop in range(1, chips):
            chip_copy(number, hop).start()
        core_copy(number).start()
    own_copy.wait()

    def arrive(number):
        for hop in range(1, chips):
            chip_copy(number, hop).wait_recv()
            pass_copy(number, hop).start()

    def head_scale(values, gain_ref):
        mean_square = jnp.mean(values * values, axis=-1, keepdims=True)
        return (values * lax.rsqrt(mean_square + NORM_EPSILON) * gain_ref[...]).astype(jnp.bfloat16)

    def head_copy(number, head, slot, owner):
        cols = pl.ds(0, 2 * hd if number == 0 else 3 * hd)
        return pltpu.make_async_remote_copy(
            src_ref=staged.at[head, span(number), cols],
            dst_ref=out.at[slot, me, span(number), cols],
            send_sem=send_sem.at[number, head],
            recv_sem=recv_sem.at[number, slot, me],
            device_id={"seq": owner}, device_id_type=MESH,
        )

    def local_copy(number, head, slot):
        cols = pl.ds(0, 2 * hd if number == 0 else 3 * hd)
        return pltpu.make_async_copy(
            staged.at[head, span(number), cols], out.at[slot, me, span(number), cols],
            local_sem.at[number, slot],
        )

    odd = core
    arrive(0)
    for number in range(chunks):
        here = span(number)
        count = here.size
        core_copy(number).wait_recv()
        for hop in range(1, chips):
            pass_copy(number, hop).wait_recv()
        if number + 1 < chunks and number > 0:
            arrive(number + 1)
        shift, gain = (3, 4) if number == 0 else (0, 1)
        pieces = [gathered[t, here, :].astype(jnp.float32) for t in range(size)]
        total = sum(jnp.sum(p, axis=-1, keepdims=True) for p in pieces)
        mean = total / width
        square = sum(jnp.sum((p - mean) * (p - mean), axis=-1, keepdims=True) for p in pieces)
        scale = lax.rsqrt(square / width + NORM_EPSILON)
        for t in range(size):
            cols = slice(t * part, (t + 1) * part)
            p = gathered[t, here, :].astype(jnp.float32)
            normed[:count, cols] = (
                (p - mean) * scale * (1.0 + mod_ref[gain : gain + 1, cols])
                + mod_ref[shift : shift + 1, cols]
            ).astype(jnp.bfloat16)
        if number < 2:
            weight_copies[number].wait()
        for kind in range(2 if number == 0 else 3):
            weight = wtxt.at[kind] if number == 0 else wimg.at[(kind + 1) % 3]
            product = jnp.dot(normed[:count, :], weight[...], preferred_element_type=jnp.float32)
            for head in range(heads):
                values = product[:, head * hd : (head + 1) * hd]
                if kind == 1:
                    values = values.astype(jnp.bfloat16)
                else:
                    values = head_scale(values, kgain_ref if kind == 0 else qgain_ref)
                staged[head, here, kind * hd : (kind + 1) * hd] = values
        for head in range(heads):
            owner, slot = head_owner(jnp.int32(head), ranks, heads, odd)

            @pl.when(owner == me)
            def _():
                local_copy(number, head, slot).start()

            @pl.when(owner != me)
            def _():
                head_copy(number, head, slot, owner).start()

        if number == 0:
            arrive(1)

    for t in range(size):
        mine_rows = own_ref.shape[0]
        own_ref[:, t * part : (t + 1) * part] = gathered[
            t, pl.ds(local_txt + slot_t * mine_rows, mine_rows), :
        ]

    mine = first_head(me + 1, ranks, heads, odd) - first_head(me, ranks, heads, odd)
    for number in range(chunks):
        core_copy(number).wait_send()
        for hop in range(1, chips):
            chip_copy(number, hop).wait_send()
            pass_copy(number, hop).wait_send()
        for head in range(heads):
            owner, slot = head_owner(jnp.int32(head), ranks, heads, odd)

            @pl.when(owner != me)
            def _():
                head_copy(number, head, slot, owner).wait_send()

        for slot in range(slots):
            @pl.when(slot < mine)
            def _():
                local_copy(number, 0, slot).wait()
                for hop in range(1, ranks):
                    peer = lax.rem(me + hop, ranks)
                    cols = pl.ds(0, 2 * hd if number == 0 else 3 * hd)
                    pltpu.make_async_remote_copy(
                        src_ref=staged.at[0, span(number), cols],
                        dst_ref=out.at[slot, peer, span(number), cols],
                        send_sem=send_sem.at[number, 0],
                        recv_sem=recv_sem.at[number, slot, peer],
                        device_id={"seq": peer}, device_id_type=MESH,
                    ).wait_recv()


def project(ranks, size, heads, local_txt, joined, modrows, wimg, wtxt, query_gain, key_gain):
    hd = query_gain.shape[0]
    rows, part = joined.shape
    width = size * part
    slots = -(-heads // ranks)
    local_img = rows - local_txt
    chunk = 128 if local_img % 128 == 0 else local_img
    chunks = 1 + local_img // chunk
    chips = size // 2
    vmem = pl.BlockSpec(memory_space=pltpu.VMEM)
    anywhere = pl.BlockSpec(memory_space=pl.ANY)
    dma = pltpu.SemaphoreType.DMA
    return pl.pallas_call(
        functools.partial(project_kernel, ranks, size, heads, local_txt, chunk),
        out_shape=(
            jax.ShapeDtypeStruct((slots, ranks, rows, 3 * hd), jnp.bfloat16),
            jax.ShapeDtypeStruct((local_img // size, width), jnp.bfloat16),
        ),
        in_specs=[vmem, vmem, anywhere, anywhere, vmem, vmem],
        out_specs=(anywhere, vmem),
        scratch_shapes=[
            pltpu.VMEM((size, rows, part), jnp.bfloat16),
            pltpu.VMEM((max(chunk, local_txt), width), jnp.bfloat16),
            pltpu.VMEM((heads, rows, 3 * hd), jnp.bfloat16),
            pltpu.VMEM(wimg.shape, jnp.bfloat16),
            pltpu.VMEM((2,) + wtxt.shape[1:], jnp.bfloat16),
            dma((2,)),
            dma((chunks, chips)),
            dma((chunks, chips)),
            dma((chunks,)),
            dma((chunks,)),
            dma((chunks, chips)),
            dma((chunks, chips)),
            dma,
            dma((chunks, heads)),
            dma((chunks, slots, ranks)),
            dma((chunks, slots)),
        ],
        compiler_params=pltpu.CompilerParams(
            collective_id=0, has_side_effects=True, vmem_limit_bytes=VMEM_LIMIT
        ),
    )(joined, modrows, wimg, wtxt, query_gain[None, :], key_gain[None, :])


def attend_kernel(
    ranks, heads, qkv_ref, valid_ref, out_ref, buf, send_sem, recv_sem, local_sem
):
    me = lax.axis_index("seq")
    odd = lax.rem(lax.axis_index("tensor"), 2)
    meet("seq", ranks, me)
    slots, _, local_img, hd = buf.shape
    local_txt = qkv_ref.shape[2] - local_img
    start = first_head(me, ranks, heads, odd)
    mine = first_head(me + 1, ranks, heads, odd) - start
    scale = math.log2(math.e) / math.sqrt(hd)
    tile = min(256, local_img)

    def columns(head):
        return out_ref.at[:, pl.ds(pl.multiple_of(head * hd, hd), hd)]

    def back(peer, slot):
        return pltpu.make_async_remote_copy(
            src_ref=buf.at[slot, peer],
            dst_ref=columns(start + slot),
            send_sem=send_sem.at[slot, peer],
            recv_sem=recv_sem.at[start + slot],
            device_id={"seq": peer},
            device_id_type=MESH,
        )

    def place(number):
        return number // ranks, lax.rem(me + 1 + lax.rem(number, ranks), ranks)

    def ship(number):
        slot, peer = place(number)

        @pl.when((slot < mine) & (peer != me))
        def _():
            back(peer, slot).start()

        @pl.when((slot < mine) & (peer == me))
        def _():
            pltpu.make_async_copy(
                buf.at[slot, me], columns(start + slot), local_sem.at[slot]
            ).start()

    def one(number, carry):
        slot, peer = place(number)

        @pl.when(slot < mine)
        def _():
            for low in range(0, local_img, tile):
                queries = qkv_ref[slot, peer, local_txt + low : local_txt + low + tile, 2 * hd :]
                total = jnp.zeros((tile, hd), jnp.float32)
                denominator = jnp.zeros((tile, 1), jnp.float32)
                for block in range(ranks):
                    scores = lax.dot_general(
                        queries, qkv_ref[slot, block, :, :hd], (((1,), (1,)), ((), ())),
                        preferred_element_type=jnp.float32,
                    )
                    weights = jnp.exp2(scores * scale) * valid_ref[block]
                    denominator = denominator + jnp.sum(weights, axis=-1, keepdims=True)
                    total = total + jnp.dot(
                        weights.astype(jnp.bfloat16), qkv_ref[slot, block, :, hd : 2 * hd],
                        preferred_element_type=jnp.float32,
                    )
                buf[slot, peer, low : low + tile, :] = (total / denominator).astype(jnp.bfloat16)

        @pl.when(number > 0)
        def _():
            ship(number - 1)

        return carry

    lax.fori_loop(0, slots * ranks, one, 0)
    ship(slots * ranks - 1)
    for slot in range(slots):
        @pl.when(slot < mine)
        def _():
            pltpu.make_async_copy(
                buf.at[slot, me], columns(start + slot), local_sem.at[slot]
            ).wait()
            for hop in range(1, ranks):
                back(lax.rem(me + hop, ranks), slot).wait_send()

    for head in range(heads):
        owner, slot = head_owner(jnp.int32(head), ranks, heads, odd)

        @pl.when(owner != me)
        def _():
            pltpu.make_async_remote_copy(
                src_ref=buf.at[0, 0], dst_ref=columns(head), send_sem=send_sem.at[0, 0],
                recv_sem=recv_sem.at[head], device_id={"seq": owner}, device_id_type=MESH,
            ).wait_recv()


def attend(ranks, heads, local_img, qkv, valid):
    slots, hd = qkv.shape[0], qkv.shape[3] // 3
    vmem = pl.BlockSpec(memory_space=pltpu.VMEM)
    return pl.pallas_call(
        functools.partial(attend_kernel, ranks, heads),
        out_shape=jax.ShapeDtypeStruct((local_img, heads * hd), jnp.bfloat16),
        in_specs=[vmem] * 2,
        out_specs=pl.BlockSpec(memory_space=pl.ANY),
        scratch_shapes=[
            pltpu.VMEM((slots, ranks, local_img, hd), jnp.bfloat16),
            pltpu.SemaphoreType.DMA((slots, ranks)),
            pltpu.SemaphoreType.DMA((heads,)),
            pltpu.SemaphoreType.DMA((slots,)),
        ],
        compiler_params=pltpu.CompilerParams(
            collective_id=1, has_side_effects=True, vmem_limit_bytes=VMEM_LIMIT
        ),
    )(qkv, valid)


def reduce_kernel(
    size, att_ref, w_ref, out_ref, first, first_in, second, second_in, sems1, sems2
):
    me = lax.axis_index("tensor")
    core = lax.rem(me, 2)
    chip = me // 2
    chips = size // 2
    partner = 2 * chip + 1 - core
    rows = att_ref.shape[0] // size

    barrier = pltpu.get_barrier_semaphore()
    pl.semaphore_signal(barrier, inc=1, device_id={"tensor": partner}, device_id_type=MESH)
    for hop in range(1, chips):
        pl.semaphore_signal(
            barrier, inc=1, device_id={"tensor": 2 * lax.rem(chip + hop, chips) + core},
            device_id_type=MESH,
        )
    pl.semaphore_wait(barrier, chips)

    def partial(owner):
        block = att_ref[pl.ds(pl.multiple_of(owner * rows, rows), rows), :]
        return jnp.dot(block, w_ref[...], preferred_element_type=jnp.float32)

    def to_partner(hop):
        return pltpu.make_async_remote_copy(
            src_ref=first.at[hop], dst_ref=first_in.at[hop],
            send_sem=sems1.at[0, hop], recv_sem=sems1.at[1, hop],
            device_id={"tensor": partner}, device_id_type=MESH,
        )

    def to_chip(hop):
        return pltpu.make_async_remote_copy(
            src_ref=second.at[hop], dst_ref=second_in.at[hop],
            send_sem=sems2.at[0, hop], recv_sem=sems2.at[1, hop],
            device_id={"tensor": 2 * lax.rem(chip + hop, chips) + core}, device_id_type=MESH,
        )

    order = list(range(1, chips)) + [0]
    for hop in order:
        target = lax.rem(chip + hop, chips)
        first[hop] = partial(2 * target + 1 - core).astype(jnp.bfloat16)
        own = partial(2 * target + core)
        to_partner(hop).start()
        to_partner(hop).wait_recv()
        total = own + first_in[hop].astype(jnp.float32)
        if hop:
            second[hop] = total.astype(jnp.bfloat16)
            to_chip(hop).start()
        else:
            out_ref[...] = total
    for hop in range(1, chips):
        to_chip(hop).wait_recv()
        out_ref[...] += second_in[hop].astype(jnp.float32)
    for hop in range(chips):
        to_partner(hop).wait_send()
        if hop:
            to_chip(hop).wait_send()


def project_reduce(size, attended, image_out):
    tokens, width = attended.shape[0], image_out.shape[1]
    rows, chips = tokens // size, size // 2
    vmem = pl.BlockSpec(memory_space=pltpu.VMEM)
    stack = pltpu.VMEM((chips, rows, width), jnp.bfloat16)
    return pl.pallas_call(
        functools.partial(reduce_kernel, size),
        out_shape=jax.ShapeDtypeStruct((rows, width), jnp.float32),
        in_specs=[vmem] * 2,
        out_specs=vmem,
        scratch_shapes=[
            stack, stack, stack, stack,
            pltpu.SemaphoreType.DMA((2, chips)),
            pltpu.SemaphoreType.DMA((2, chips)),
        ],
        compiler_params=pltpu.CompilerParams(
            collective_id=2, has_side_effects=True, vmem_limit_bytes=VMEM_LIMIT
        ),
    )(attended, image_out)


def total_kernel(sizes, x_ref, out_ref, *scratch):
    me = {axis: lax.axis_index(axis) for axis, _ in sizes}
    barrier = pltpu.get_barrier_semaphore()
    count = 0
    for axis, size in sizes:
        for hop in range(1, size):
            pl.semaphore_signal(
                barrier, inc=1, device_id={axis: lax.rem(me[axis] + hop, size)},
                device_id_type=MESH,
            )
            count += 1
    pl.semaphore_wait(barrier, count)
    held = x_ref
    for number, (axis, size) in enumerate(sizes):
        slots, total, sems = scratch[3 * number : 3 * number + 3]
        copies = []
        for hop in range(1, size):
            copy = pltpu.make_async_remote_copy(
                src_ref=held, dst_ref=slots.at[hop], send_sem=sems.at[0, hop],
                recv_sem=sems.at[1, hop],
                device_id={axis: lax.rem(me[axis] + hop, size)}, device_id_type=MESH,
            )
            copy.start()
            copies.append(copy)
        sum_now = held[...]
        for hop, copy in enumerate(copies, 1):
            copy.wait()
            sum_now = sum_now + slots[hop]
        total[...] = sum_now
        held = total
    out_ref[...] = held[...]


def total_sum(sizes, tile):
    vmem = pl.BlockSpec(memory_space=pltpu.VMEM)
    scratch = []
    for _, size in sizes:
        scratch += [
            pltpu.VMEM((size,) + tile.shape, jnp.float32),
            pltpu.VMEM(tile.shape, jnp.float32),
            pltpu.SemaphoreType.DMA((2, size)),
        ]
    return pl.pallas_call(
        functools.partial(total_kernel, sizes),
        out_shape=jax.ShapeDtypeStruct(tile.shape, jnp.float32),
        in_specs=[vmem],
        out_specs=vmem,
        scratch_shapes=scratch,
        compiler_params=pltpu.CompilerParams(collective_id=3, has_side_effects=True),
    )(tile)


def shards(
    image_states, text_states, image_qkv, text_qkv, image_out, final_weight, query_gain, key_gain,
    modulation, latent, old_velocity, rollout_noise, group_ids, text_lengths, step_ids,
):
    local_img = image_states.shape[1]
    local_txt = text_states.shape[1]
    hd = query_gain.shape[0]
    heads = image_qkv.shape[2] // hd
    total_steps = modulation.shape[0]
    ranks = lax.axis_size("seq")
    size = lax.axis_size("tensor")
    group = group_ids[0]
    modrows = modulation[step_ids[0]]
    length = text_lengths[group]
    joined = jnp.concatenate([text_states[group], image_states[0]], axis=0)
    qkv, own_rows = project(
        ranks, size, heads, local_txt, joined, modrows,
        jnp.transpose(image_qkv, (1, 0, 2)), jnp.transpose(text_qkv, (1, 0, 2)),
        query_gain, key_gain,
    )
    place = jnp.arange(local_txt + local_img, dtype=jnp.int32)[None, :]
    text_pos = jnp.arange(ranks, dtype=jnp.int32)[:, None] * local_txt + place
    valid = ((place >= local_txt) | (text_pos < length)).astype(jnp.float32)[:, None, :]
    attended = attend(ranks, heads, local_img, qkv, valid)
    summed = project_reduce(size, attended, image_out)
    resid = own_rows.astype(jnp.float32) + modrows[2] * summed
    final_normed = (layer_norm(resid) * (1.0 + modrows[6]) + modrows[5]).astype(jnp.bfloat16)
    velocity = jnp.dot(final_normed, final_weight, preferred_element_type=jnp.float32)[None]
    flow_time, step_delta, noise_sigma, spread = plan(step_ids, total_steps)
    flow_e = flow_time[:, None, None]
    sigma_e = noise_sigma[:, None, None]
    step_mean = drift_mean(latent, velocity, flow_e, step_delta, sigma_e)
    mean_old = drift_mean(latent, old_velocity.astype(jnp.float32), flow_e, step_delta, sigma_e)
    shifted = rollout_noise + (mean_old - step_mean) / spread[:, None, None]
    partial_ratio = jnp.sum(rollout_noise * rollout_noise - shifted * shifted) * 0.5
    tile = jnp.broadcast_to(partial_ratio, (8, 128))
    ratio_total = total_sum((("tensor", size), ("seq", ranks)), tile)[0, :1]
    elements = latent.shape[1] * ranks * size * latent.shape[2]
    return (step_mean, ratio_total / elements)


def solution(mesh):
    placed = (
        P("dp", "seq", "tensor"),
        P(None, "seq", "tensor"),
        P(None, None, "tensor"),
        P(None, None, "tensor"),
        P("tensor", None),
        P(),
        P(),
        P(),
        P(),
        P("dp", ("seq", "tensor"), None),
        P("dp", ("seq", "tensor"), None),
        P("dp", ("seq", "tensor"), None),
        P("dp"),
        P(),
        P("dp"),
    )
    return jax.shard_map(
        shards,
        mesh=mesh,
        in_specs=placed,
        out_specs=(P("dp", ("seq", "tensor"), None), P("dp")),
        check_vma=False,
    )
```
